32 devices in a mesh: gx: 16 (over z, y, core), gy: 2 (over x).
Axes of the slice: x: 2, y: 2, z: 4, core: 2. Of those that a mesh axis runs over, the one named last changes fastest.
Arguments:
- prognostic_values: float32 [3, 6, 2048, 1024], P(None, None, 'gx', 'gy'), may hold values from -6 to 6
- forcing_host_values: bfloat16 [3, 6, 2048, 1024], P(None, None, 'gx', 'gy'), may hold values from -6 to 6
- strength: float32 [3, 6], replicated, may hold values from 50 to 200
- level_height: float32 [3], replicated, may hold values from 0.2 to 3
- pbl_height: float32 [2048, 1024], P('gx', 'gy'), may hold values from 0.2 to 3
Outputs:
- tendency: bfloat16 [3, 6, 2048, 1024], P(None, None, 'gx', 'gy')
- energy: float32 [3, 6], replicated
The draws below stay inside these ranges and needn't reach their ends.
All inputs are finite; a program needn't handle non-finite values.
Results may differ from the reference program's by a relative error of at most 0.001.
Values sent between devices are 32-bit elements; how exact they have to be, the bound alone decides.
A program may use at most 64 MiB of HBM per device.

```python
import math
import jax
import jax.numpy as jnp
from jax import lax

KX = 32
KY = 32
VARS = 6
LEV = 3
NX = 2048
NY = 1024


def level_of(rng, extent, cuts, low, high):
    def one(dim, shards_of):
        steps = jax.random.uniform(jax.random.fold_in(jax.random.fold_in(rng, 6), dim), (shards_of,), jnp.float32, low / len(cuts), high / len(cuts))
        return jnp.repeat(jnp.exp(steps), extent[dim] // shards_of).reshape((-1,) + (1,) * (len(extent) - dim - 1))

    gain = one(*cuts[0])
    for cut in cuts[1:]:
        gain = gain * one(*cut)
    return gain


def gaussian(own_key, extent, deviation, most, shards=(), dtype=jnp.bfloat16):
    level = level_of(own_key, extent, shards, -0.22, 0.18) if shards else 1.0
    values = jax.random.normal(own_key, extent, jnp.float32) * deviation * level
    return jnp.minimum(jnp.maximum(values, -most), most).astype(dtype)


def setup_inputs(seed: int = 0) -> dict:
    seeds = jax.random.split(jax.random.key(seed), 6)
    prognostic_values = gaussian(seeds[0], (LEV, VARS, NX, NY), 1.0, 6.0, ((2, 16), (3, 2)), jnp.float32)
    forcing_host_values = gaussian(seeds[1], (LEV, VARS, NX, NY), 1.0, 6.0, ((2, 16), (3, 2)))
    strength = jnp.clip(jnp.exp(jax.random.uniform(seeds[2], (LEV, VARS), jnp.float32, math.log(50.0), math.log(200.0))), 50.0, 200.0)
    level_height = jnp.clip(jax.random.uniform(seeds[3], (LEV,), jnp.float32, 0.2, 3.0), 0.2, 3.0)
    pbl_height = jnp.clip(0.2 + 2.8 * jax.random.uniform(seeds[4], (NX, NY), jnp.float32) ** level_of(seeds[4], (NX, NY), ((0, 16), (1, 2)), -0.2, 0.2), 0.2, 3.0)
    return {"prognostic_values": prognostic_values, "forcing_host_values": forcing_host_values, "strength": strength, "level_height": level_height, "pbl_height": pbl_height}


ramp_depth = 0.25

def cosine_table(total, modes, start, count):
    index = (start + jnp.arange(count)).astype(jnp.float32)
    waves = jnp.arange(modes).astype(jnp.float32)
    scales = jnp.where(waves == 0.0, jnp.sqrt(1.0 / total), jnp.sqrt(2.0 / total)).astype(jnp.float32)
    return scales[None, :] * jnp.cos(jnp.pi * (index[:, None] + 0.5) * waves[None, :] / total)

def reference(prognostic_values, forcing_host_values, strength, level_height, pbl_height):
    meridional_cosines = cosine_table(NX, KX, 0, NX)
    col_basis = cosine_table(NY, KY, 0, NY)
    largest_wavenumber = lax.Precision.HIGHEST

    def one_level(items):
        model, driver, gains, altitude_factor = items
        diff = driver.astype(jnp.float32) - model
        part = jnp.einsum('vij,jb->vib', diff, col_basis, precision=largest_wavenumber)
        mode_factors = jnp.einsum('wl,ywg->ylg', meridional_cosines, part, precision=largest_wavenumber)
        restored_fields = jnp.einsum('ky,jyp->jkp', meridional_cosines, mode_factors, precision=largest_wavenumber)
        recon = jnp.einsum('vib,jb->vij', restored_fields, col_basis, precision=largest_wavenumber)
        damping_share = 1.0 / (1.0 + jnp.exp(-(altitude_factor - pbl_height) / ramp_depth))
        tend = (gains[:, None, None] * damping_share[None] * recon).astype(jnp.bfloat16)
        energy = lax.optimization_barrier(jnp.sum(recon * recon, axis=(1, 2))) / (KX * KY)
        return (tend, energy)
    tendency, energy = lax.map(one_level, (prognostic_values, forcing_host_values, strength, level_height))
    return (tendency, energy)
```

```python
import functools
import math

import jax
import jax.numpy as jnp
from jax import lax
from jax.experimental import pallas as pl
from jax.experimental.pallas import tpu as pltpu
from jax.sharding import PartitionSpec as P

KX = 32
KY = 32
RAMP_DEPTH = 0.25
LANES = 128
SUB = 8
MESH = pl.DeviceIdType.MESH

F32 = jnp.float32
BF16 = jnp.bfloat16

SINE = [(-1.0) ** k * (math.pi / 2) ** (2 * k + 1) / math.factorial(2 * k + 1) for k in range(7)]


def basis(total, place, wave):
    turns = (2.0 * place + 1.0) * wave
    rest = turns - (4.0 * total) * jnp.floor(turns * (1.0 / (4.0 * total)))
    t = (jnp.abs(rest - 2.0 * total) - total) * (1.0 / total)
    t2 = t * t
    poly = jnp.full(t.shape, SINE[-1], F32)
    for c in SINE[-2::-1]:
        poly = poly * t2 + c
    scale = jnp.where(wave == 0.0, math.sqrt(1.0 / total), math.sqrt(2.0 / total))
    return scale * (poly * t)


def iota(shape, dim):
    return lax.broadcasted_iota(jnp.int32, shape, dim)


def split(x):
    hi = x.astype(BF16)
    return hi, (x - hi.astype(F32)).astype(BF16)


def group_masks(rows):
    lane = iota((rows, LANES), 1) // KY
    return [lane == g for g in range(LANES // KY)]


def analysis_kernel(
    dims, prog_hbm, forc_hbm, coef_ref,
    prog, forc, part, mine, got_in, total, got_out, full,
    prog_sem, forc_sem, in_send, in_recv, out_send, out_recv, all_send, all_recv,
):
    gx, gy, n_mid, chunk = dims
    fields, rows, cols = prog.shape
    n_chunks = fields // chunk
    groups = KX // SUB
    n_in, n_out = n_mid * gy, gx // n_mid
    ix, iy = lax.axis_index("gx"), lax.axis_index("gy")
    outer, mid = ix // n_mid, lax.rem(ix, n_mid)
    me = mid * gy + iy

    def fetch(c):
        span = pl.ds(c * chunk, chunk)
        return (
            pltpu.make_async_copy(prog_hbm.at[span], prog.at[span], prog_sem.at[c]),
            pltpu.make_async_copy(forc_hbm.at[span], forc.at[span], forc_sem.at[c]),
        )

    for c in range(n_chunks):
        for copy in fetch(c):
            copy.start()

    def inner_peer(d):
        other = lax.rem(me + d, n_in)
        return other, (outer * n_mid + other // gy, lax.rem(other, gy))

    def outer_peer(d):
        return (lax.rem(outer + d, n_out) * n_mid + mid, iy)

    barrier = pltpu.get_barrier_semaphore()
    for d in range(1, n_in):
        pl.semaphore_signal(barrier, inc=1, device_id=inner_peer(d)[1], device_id_type=MESH)
    for d in range(1, n_out):
        pl.semaphore_signal(barrier, inc=1, device_id=outer_peer(d), device_id_type=MESH)

    row = basis(
        rows * gx,
        (ix * rows + iota((KX, rows), 1)).astype(F32),
        iota((KX, rows), 0).astype(F32),
    )
    row_hi, row_lo = split(row)
    row_lhs = jnp.concatenate([row_hi, row_lo], axis=0)
    row_lhs = jnp.concatenate([row_lhs, row_lhs], axis=1)
    col = basis(
        cols * gy,
        (iy * cols + iota((cols, LANES), 0)).astype(F32),
        lax.rem(iota((cols, LANES), 1), KY).astype(F32),
    )
    col_rhs = jnp.concatenate(split(col), axis=1)

    def one_chunk(c, carry):
        for copy in fetch(c):
            copy.wait()
        for k in range(chunk):
            f = c * chunk + k
            diff = forc[f].astype(F32) - prog[f]
            rhs = jnp.concatenate(split(diff), axis=0)
            both = jnp.dot(row_lhs, rhs, preferred_element_type=F32)
            both = both[:KX] + both[KX:]
            for g in range(groups):
                part[g, f] = both[g * SUB:(g + 1) * SUB]
        return carry

    lax.fori_loop(0, n_chunks, one_chunk, 0)

    hi, lo = split(part[...].reshape(groups * fields * SUB, cols))
    both = jnp.dot(hi, col_rhs, preferred_element_type=F32) + jnp.dot(
        lo, col_rhs, preferred_element_type=F32
    )
    both = both[:, :LANES] + both[:, LANES:]
    size = fields * SUB
    coef = both[:size]
    for g, mask in list(enumerate(group_masks(size)))[1:]:
        coef = jnp.where(mask, both[g * size:(g + 1) * size], coef)
    slots = mine.shape[0]
    for f in range(slots * n_in):
        if f < fields:
            mine[f // n_in, f % n_in] = coef[f * SUB:(f + 1) * SUB]
        else:
            mine[f // n_in, f % n_in] = jnp.zeros((SUB, LANES), F32)

    pl.semaphore_wait(barrier, n_in - 1 + n_out - 1)

    copies = []
    for d in range(1, n_in):
        other, device = inner_peer(d)
        copies.append(pltpu.make_async_remote_copy(
            src_ref=mine.at[:, other], dst_ref=got_in.at[d - 1],
            send_sem=in_send.at[d - 1], recv_sem=in_recv.at[d - 1],
            device_id=device, device_id_type=MESH,
        ))
        copies[-1].start()
    acc = mine[:, me]
    for d, copy in enumerate(copies):
        copy.wait_recv()
        acc = acc + got_in[d]
    total[...] = acc
    outs = []
    for d in range(1, n_out):
        outs.append(pltpu.make_async_remote_copy(
            src_ref=total, dst_ref=got_out.at[d - 1],
            send_sem=out_send.at[d - 1], recv_sem=out_recv.at[d - 1],
            device_id=outer_peer(d), device_id_type=MESH,
        ))
        outs[-1].start()
    for d, copy in enumerate(outs):
        copy.wait_recv()
        acc = acc + got_out[d]
    full[:, me] = acc
    alls = []
    for d in range(1, n_in):
        alls.append(pltpu.make_async_remote_copy(
            src_ref=full.at[:, me], dst_ref=full.at[:, me],
            send_sem=all_send.at[d - 1], recv_sem=all_recv.at[d - 1],
            device_id=inner_peer(d)[1], device_id_type=MESH,
        ))
        alls[-1].start()
    for copy in alls:
        copy.wait_recv()
    for f in range(fields):
        coef_ref[f * SUB:(f + 1) * SUB] = full[f // n_in, f % n_in]
    for copy in copies + outs + alls:
        copy.wait_send()


def synthesis_kernel(
    dims, strength_ref, level_ref, coef_ref, pbl_ref, tend_hbm, energy_ref,
    wave, weight, tend, tend_sem,
):
    gx, gy = dims
    levels, variables, rows, cols = tend.shape
    fields = levels * variables
    groups = KX // SUB
    ix, iy = lax.axis_index("gx"), lax.axis_index("gy")

    coef = coef_ref[...]
    size = fields * SUB
    stack = jnp.concatenate([jnp.where(m, coef, 0.0) for m in group_masks(size)], axis=0)
    hi, lo = split(stack)
    lhs = jnp.concatenate([hi, lo, hi], axis=1)
    col_hi, col_lo = split(basis(
        cols * gy,
        (iy * cols + iota((LANES, cols), 1)).astype(F32),
        lax.rem(iota((LANES, cols), 0), KY).astype(F32),
    ))
    rhs = jnp.concatenate([col_hi, col_hi, col_lo], axis=0)
    wave[...] = jnp.dot(lhs, rhs, preferred_element_type=F32).reshape(
        groups, fields, SUB, cols
    )

    row_hi, row_lo = split(basis(
        rows * gx,
        (ix * rows + iota((rows, 4 * KX), 0)).astype(F32),
        lax.rem(iota((rows, 4 * KX), 1), KX).astype(F32),
    ))
    row_lhs = jnp.where(iota((rows, 4 * KX), 1) < 2 * KX, row_hi.astype(F32), row_lo.astype(F32)).astype(BF16)

    power = coef * coef
    at_row = iota((levels, variables), 0)
    at_col = iota((levels, variables), 1)
    energy = jnp.zeros((levels, variables), F32)
    for l in range(levels):
        for v in range(variables):
            f = l * variables + v
            one = jnp.sum(power[f * SUB:(f + 1) * SUB], axis=(0, 1), keepdims=True)
            energy = jnp.where((at_row == l) & (at_col == v), one, energy)
    energy_ref[...] = energy * (1.0 / (KX * KY))

    def put(l, v):
        return pltpu.make_async_copy(tend.at[l, v], tend_hbm.at[l, v], tend_sem.at[l, v])

    def one_level(l, carry):
        weight[...] = 1.0 / (1.0 + jnp.exp(-(level_ref[l] - pbl_ref[...]) / RAMP_DEPTH))
        for v in range(variables):
            f = l * variables + v
            whole = jnp.concatenate([wave[g, f] for g in range(groups)], axis=0)
            hi, lo = split(whole)
            rhs = jnp.concatenate([hi, lo, hi, lo], axis=0)
            recon = jnp.dot(row_lhs, rhs, preferred_element_type=F32)
            tend[l, v] = (strength_ref[l, v] * weight[...] * recon).astype(BF16)
            if v:
                put(l, v - 1).start()
        put(l, variables - 1).start()
        return carry

    lax.fori_loop(0, levels, one_level, 0)
    for l in range(levels):
        for v in range(variables):
            put(l, v).wait()


def per_device(gx, gy, prognostic_values, forcing_host_values, strength, level_height, pbl_height):
    levels, variables, rows, cols = prognostic_values.shape
    fields = levels * variables
    groups = KX // SUB
    n_mid = math.gcd(gx, 4)
    n_in, n_out = n_mid * gy, gx // n_mid
    slots = -(-fields // n_in)
    chunk = 3 if fields % 3 == 0 else 1
    n_chunks = fields // chunk
    anywhere = pl.BlockSpec(memory_space=pl.ANY)
    vmem = pl.BlockSpec(memory_space=pltpu.VMEM)
    smem = pl.BlockSpec(memory_space=pltpu.SMEM)
    dma = pltpu.SemaphoreType.DMA
    coef = pl.pallas_call(
        functools.partial(analysis_kernel, (gx, gy, n_mid, chunk)),
        out_shape=jax.ShapeDtypeStruct((fields * SUB, LANES), F32),
        in_specs=[anywhere, anywhere],
        out_specs=vmem,
        scratch_shapes=[
            pltpu.VMEM((fields, rows, cols), F32),
            pltpu.VMEM((fields, rows, cols), BF16),
            pltpu.VMEM((groups, fields, SUB, cols), F32),
            pltpu.VMEM((slots, n_in, SUB, LANES), F32),
            pltpu.VMEM((max(n_in - 1, 1), slots, SUB, LANES), F32),
            pltpu.VMEM((slots, SUB, LANES), F32),
            pltpu.VMEM((max(n_out - 1, 1), slots, SUB, LANES), F32),
            pltpu.VMEM((slots, n_in, SUB, LANES), F32),
            dma((n_chunks,)),
            dma((n_chunks,)),
            dma((max(n_in - 1, 1),)),
            dma((max(n_in - 1, 1),)),
            dma((max(n_out - 1, 1),)),
            dma((max(n_out - 1, 1),)),
            dma((max(n_in - 1, 1),)),
            dma((max(n_in - 1, 1),)),
        ],
        compiler_params=pltpu.CompilerParams(collective_id=0, has_side_effects=True),
        name="analysis",
    )(
        prognostic_values.reshape(fields, rows, cols),
        forcing_host_values.reshape(fields, rows, cols),
    )
    tendency, energy = pl.pallas_call(
        functools.partial(synthesis_kernel, (gx, gy)),
        out_shape=(
            jax.ShapeDtypeStruct((levels, variables, rows, cols), BF16),
            jax.ShapeDtypeStruct((levels, variables), F32),
        ),
        in_specs=[smem, smem, vmem, vmem],
        out_specs=(anywhere, vmem),
        scratch_shapes=[
            pltpu.VMEM((groups, fields, SUB, cols), F32),
            pltpu.VMEM((rows, cols), F32),
            pltpu.VMEM((levels, variables, rows, cols), BF16),
            dma((levels, variables)),
        ],
        name="synthesis",
    )(strength, level_height, coef, pbl_height)
    return tendency, energy


def solution(mesh):
    return jax.shard_map(
        functools.partial(per_device, mesh.shape["gx"], mesh.shape["gy"]),
        mesh=mesh,
        in_specs=(P(None, None, "gx", "gy"), P(None, None, "gx", "gy"), P(), P(), P("gx", "gy")),
        out_specs=(P(None, None, "gx", "gy"), P()),
        check_vma=False,
    )
```

```python
import functools
import math

import jax
import jax.numpy as jnp
from jax import lax
from jax.experimental import pallas as pl
from jax.experimental.pallas import tpu as pltpu
from jax.sharding import PartitionSpec as P

KX = 32
KY = 32
RAMP_DEPTH = 0.25
LANES = 128
SUB = 8
MESH = pl.DeviceIdType.MESH

F32 = jnp.float32
BF16 = jnp.bfloat16

SINE = [(-1.0) ** k * (math.pi / 2) ** (2 * k + 1) / math.factorial(2 * k + 1) for k in range(7)]


def basis(total, place, wave):
    turns = (2.0 * place + 1.0) * wave
    rest = turns - (4.0 * total) * jnp.floor(turns * (1.0 / (4.0 * total)))
    t = (jnp.abs(rest - 2.0 * total) - total) * (1.0 / total)
    t2 = t * t
    poly = jnp.full(t.shape, SINE[-1], F32)
    for c in SINE[-2::-1]:
        poly = poly * t2 + c
    scale = jnp.where(wave == 0.0, math.sqrt(1.0 / total), math.sqrt(2.0 / total))
    return scale * (poly * t)


def iota(shape, dim):
    return lax.broadcasted_iota(jnp.int32, shape, dim)


def split(x):
    hi = x.astype(BF16)
    return hi, (x - hi.astype(F32)).astype(BF16)


def group_masks(rows):
    lane = iota((rows, LANES), 1) // KY
    return [lane == g for g in range(LANES // KY)]


def analysis_kernel(
    dims, prog_hbm, forc_hbm, strength_hbm, level_hbm, pbl_hbm,
    coef_ref, scale_ref, weight_ref, row_ref, col_ref,
    strength, level, pbl, prog, forc, part, mine, got_in, total, got_out, full,
    prog_sem, forc_sem, aux_sem, in_send, in_recv, out_send, out_recv, all_send, all_recv,
):
    gx, gy, n_mid, chunk = dims
    fields, rows, cols = prog.shape
    n_chunks = fields // chunk
    groups = KX // SUB
    n_in, n_out = n_mid * gy, gx // n_mid
    ix, iy = lax.axis_index("gx"), lax.axis_index("gy")
    outer, mid = ix // n_mid, lax.rem(ix, n_mid)
    me = mid * gy + iy

    def fetch(c):
        span = pl.ds(c * chunk, chunk)
        return (
            pltpu.make_async_copy(prog_hbm.at[span], prog.at[span], prog_sem.at[c]),
            pltpu.make_async_copy(forc_hbm.at[span], forc.at[span], forc_sem.at[c]),
        )

    for c in range(n_chunks):
        for copy in fetch(c):
            copy.start()
    aux = [
        pltpu.make_async_copy(pbl_hbm, pbl, aux_sem.at[0]),
        pltpu.make_async_copy(strength_hbm, strength, aux_sem.at[1]),
        pltpu.make_async_copy(level_hbm, level, aux_sem.at[2]),
    ]
    for copy in aux:
        copy.start()

    def inner_peer(d):
        other = lax.rem(me + d, n_in)
        return other, (outer * n_mid + other // gy, lax.rem(other, gy))

    def outer_peer(d):
        return (lax.rem(outer + d, n_out) * n_mid + mid, iy)

    barrier = pltpu.get_barrier_semaphore()
    for d in range(1, n_in):
        pl.semaphore_signal(barrier, inc=1, device_id=inner_peer(d)[1], device_id_type=MESH)
    for d in range(1, n_out):
        pl.semaphore_signal(barrier, inc=1, device_id=outer_peer(d), device_id_type=MESH)

    row = basis(
        rows * gx,
        (ix * rows + iota((KX, rows), 1)).astype(F32),
        iota((KX, rows), 0).astype(F32),
    )
    row_hi, row_lo = split(row)
    row_lhs = jnp.concatenate([row_hi, row_lo], axis=0)
    row_lhs = jnp.concatenate([row_lhs, row_lhs], axis=1)
    col = basis(
        cols * gy,
        (iy * cols + iota((cols, LANES), 0)).astype(F32),
        lax.rem(iota((cols, LANES), 1), KY).astype(F32),
    )
    col_rhs = jnp.concatenate(split(col), axis=1)

    def one_chunk(c, carry):
        for copy in fetch(c):
            copy.wait()
        for k in range(chunk):
            f = c * chunk + k
            diff = forc[f].astype(F32) - prog[f]
            rhs = jnp.concatenate(split(diff), axis=0)
            both = jnp.dot(row_lhs, rhs, preferred_element_type=F32)
            both = both[:KX] + both[KX:]
            for g in range(groups):
                part[g, f] = both[g * SUB:(g + 1) * SUB]
        return carry

    lax.fori_loop(0, n_chunks, one_chunk, 0)

    hi, lo = split(part[...].reshape(groups * fields * SUB, cols))
    both = jnp.dot(hi, col_rhs, preferred_element_type=F32) + jnp.dot(
        lo, col_rhs, preferred_element_type=F32
    )
    both = both[:, :LANES] + both[:, LANES:]
    size = fields * SUB
    coef = both[:size]
    for g, mask in list(enumerate(group_masks(size)))[1:]:
        coef = jnp.where(mask, both[g * size:(g + 1) * size], coef)
    slots = mine.shape[0]
    for f in range(slots * n_in):
        if f < fields:
            mine[f // n_in, f % n_in] = coef[f * SUB:(f + 1) * SUB]
        else:
            mine[f // n_in, f % n_in] = jnp.zeros((SUB, LANES), F32)

    pl.semaphore_wait(barrier, n_in - 1 + n_out - 1)

    copies = []
    for d in range(1, n_in):
        other, device = inner_peer(d)
        copies.append(pltpu.make_async_remote_copy(
            src_ref=mine.at[:, other], dst_ref=got_in.at[d - 1],
            send_sem=in_send.at[d - 1], recv_sem=in_recv.at[d - 1],
            device_id=device, device_id_type=MESH,
        ))
        copies[-1].start()
    for copy in aux:
        copy.wait()
    levels, variables = strength.shape
    for l in range(levels):
        weight_ref[l] = 1.0 / (1.0 + jnp.exp(-(level[l] - pbl[...]) / RAMP_DEPTH))
        for v in range(variables):
            f = l * variables + v
            scale_ref[f * SUB:(f + 1) * SUB] = jnp.full((SUB, LANES), strength[l, v], F32)
    col_hi, col_lo = split(basis(
        cols * gy,
        (iy * cols + iota((LANES, cols), 1)).astype(F32),
        lax.rem(iota((LANES, cols), 0), KY).astype(F32),
    ))
    col_ref[...] = jnp.concatenate([col_hi, col_hi, col_lo], axis=0)
    row_hi, row_lo = split(basis(
        rows * gx,
        (ix * rows + iota((rows, 4 * KX), 0)).astype(F32),
        lax.rem(iota((rows, 4 * KX), 1), KX).astype(F32),
    ))
    row_ref[...] = jnp.where(
        iota((rows, 4 * KX), 1) < 2 * KX, row_hi.astype(F32), row_lo.astype(F32)
    ).astype(BF16)

    acc = mine[:, me]
    for d, copy in enumerate(copies):
        copy.wait_recv()
        acc = acc + got_in[d]
    total[...] = acc
    outs = []
    for d in range(1, n_out):
        outs.append(pltpu.make_async_remote_copy(
            src_ref=total, dst_ref=got_out.at[d - 1],
            send_sem=out_send.at[d - 1], recv_sem=out_recv.at[d - 1],
            device_id=outer_peer(d), device_id_type=MESH,
        ))
        outs[-1].start()
    for d, copy in enumerate(outs):
        copy.wait_recv()
        acc = acc + got_out[d]
    full[:, me] = acc
    alls = []
    for d in range(1, n_in):
        alls.append(pltpu.make_async_remote_copy(
            src_ref=full.at[:, me], dst_ref=full.at[:, me],
            send_sem=all_send.at[d - 1], recv_sem=all_recv.at[d - 1],
            device_id=inner_peer(d)[1], device_id_type=MESH,
        ))
        alls[-1].start()
    for copy in alls:
        copy.wait_recv()
    for f in range(fields):
        coef_ref[f * SUB:(f + 1) * SUB] = full[f // n_in, f % n_in]
    for copy in copies + outs + alls:
        copy.wait_send()


def synthesis_kernel(
    coef_ref, scale_ref, weight_ref, row_ref, col_ref, tend_hbm, energy_ref, wave, tend, tend_sem,
):
    levels, variables, rows, cols = tend.shape
    fields = levels * variables
    groups = KX // SUB

    coef = coef_ref[...]
    size = fields * SUB
    scaled = coef * scale_ref[...]
    stack = jnp.concatenate([jnp.where(m, scaled, 0.0) for m in group_masks(size)], axis=0)
    hi, lo = split(stack)
    lhs = jnp.concatenate([hi, lo, hi], axis=1)
    wave[...] = jnp.dot(lhs, col_ref[...], preferred_element_type=F32).reshape(
        groups, fields, SUB, cols
    )

    def put(l, v):
        return pltpu.make_async_copy(tend.at[l, v], tend_hbm.at[l, v], tend_sem.at[l, v])

    def one_level(l, carry):
        for v in range(variables):
            f = l * variables + v
            whole = jnp.concatenate([wave[g, f] for g in range(groups)], axis=0)
            hi, lo = split(whole)
            rhs = jnp.concatenate([hi, lo, hi, lo], axis=0)
            recon = jnp.dot(row_ref[...], rhs, preferred_element_type=F32)
            tend[l, v] = (weight_ref[l] * recon).astype(BF16)
            if v:
                put(l, v - 1).start()
        put(l, variables - 1).start()
        return carry

    lax.fori_loop(0, levels, one_level, 0)

    power = coef * coef
    at_row = iota((levels, variables), 0)
    at_col = iota((levels, variables), 1)
    energy = jnp.zeros((levels, variables), F32)
    for l in range(levels):
        for v in range(variables):
            f = l * variables + v
            one = jnp.sum(power[f * SUB:(f + 1) * SUB], axis=(0, 1), keepdims=True)
            energy = jnp.where((at_row == l) & (at_col == v), one, energy)
    energy_ref[...] = energy * (1.0 / (KX * KY))

    for l in range(levels):
        for v in range(variables):
            put(l, v).wait()


def per_device(gx, gy, prognostic_values, forcing_host_values, strength, level_height, pbl_height):
    levels, variables, rows, cols = prognostic_values.shape
    fields = levels * variables
    groups = KX // SUB
    n_mid = math.gcd(gx, 4)
    n_in, n_out = n_mid * gy, gx // n_mid
    slots = -(-fields // n_in)
    chunk = 3 if fields % 3 == 0 else 1
    n_chunks = fields // chunk
    anywhere = pl.BlockSpec(memory_space=pl.ANY)
    vmem = pl.BlockSpec(memory_space=pltpu.VMEM)
    dma = pltpu.SemaphoreType.DMA
    held = pl.pallas_call(
        functools.partial(analysis_kernel, (gx, gy, n_mid, chunk)),
        out_shape=(
            pltpu.VMEM((fields * SUB, LANES), F32),
            pltpu.VMEM((fields * SUB, LANES), F32),
            pltpu.VMEM((levels, rows, cols), F32),
            pltpu.VMEM((rows, 4 * KX), BF16),
            pltpu.VMEM((3 * LANES, cols), BF16),
        ),
        in_specs=[anywhere] * 5,
        out_specs=(vmem,) * 5,
        scratch_shapes=[
            pltpu.SMEM((levels, variables), F32),
            pltpu.SMEM((levels,), F32),
            pltpu.VMEM((rows, cols), F32),
            pltpu.VMEM((fields, rows, cols), F32),
            pltpu.VMEM((fields, rows, cols), BF16),
            pltpu.VMEM((groups, fields, SUB, cols), F32),
            pltpu.VMEM((slots, n_in, SUB, LANES), F32),
            pltpu.VMEM((max(n_in - 1, 1), slots, SUB, LANES), F32),
            pltpu.VMEM((slots, SUB, LANES), F32),
            pltpu.VMEM((max(n_out - 1, 1), slots, SUB, LANES), F32),
            pltpu.VMEM((slots, n_in, SUB, LANES), F32),
            dma((n_chunks,)),
            dma((n_chunks,)),
            dma((3,)),
            dma((max(n_in - 1, 1),)),
            dma((max(n_in - 1, 1),)),
            dma((max(n_out - 1, 1),)),
            dma((max(n_out - 1, 1),)),
            dma((max(n_in - 1, 1),)),
            dma((max(n_in - 1, 1),)),
        ],
        compiler_params=pltpu.CompilerParams(collective_id=0, has_side_effects=True),
        name="analysis",
    )(
        prognostic_values.reshape(fields, rows, cols),
        forcing_host_values.reshape(fields, rows, cols),
        strength,
        level_height,
        pbl_height,
    )
    tendency, energy = pl.pallas_call(
        synthesis_kernel,
        out_shape=(
            jax.ShapeDtypeStruct((levels, variables, rows, cols), BF16),
            jax.ShapeDtypeStruct((levels, variables), F32),
        ),
        in_specs=[vmem] * 5,
        out_specs=(anywhere, vmem),
        scratch_shapes=[
            pltpu.VMEM((groups, fields, SUB, cols), F32),
            pltpu.VMEM((levels, variables, rows, cols), BF16),
            dma((levels, variables)),
        ],
        name="synthesis",
    )(*[pltpu.with_memory_space_constraint(x, pltpu.VMEM) for x in held])
    return tendency, energy


def solution(mesh):
    return jax.shard_map(
        functools.partial(per_device, mesh.shape["gx"], mesh.shape["gy"]),
        mesh=mesh,
        in_specs=(P(None, None, "gx", "gy"), P(None, None, "gx", "gy"), P(), P(), P("gx", "gy")),
        out_specs=(P(None, None, "gx", "gy"), P()),
        check_vma=False,
    )
```

```python
import functools
import math

import jax
import jax.numpy as jnp
from jax import lax
from jax.experimental import pallas as pl
from jax.experimental.pallas import tpu as pltpu
from jax.sharding import PartitionSpec as P

KX = 32
KY = 32
RAMP_DEPTH = 0.25
LANES = 128
SUB = 8
MESH = pl.DeviceIdType.MESH

F32 = jnp.float32
BF16 = jnp.bfloat16

SINE = [(-1.0) ** k * (math.pi / 2) ** (2 * k + 1) / math.factorial(2 * k + 1) for k in range(7)]


def basis(total, place, wave):
    turns = (2.0 * place + 1.0) * wave
    rest = turns - (4.0 * total) * jnp.floor(turns * (1.0 / (4.0 * total)))
    t = (jnp.abs(rest - 2.0 * total) - total) * (1.0 / total)
    t2 = t * t
    poly = jnp.full(t.shape, SINE[-1], F32)
    for c in SINE[-2::-1]:
        poly = poly * t2 + c
    scale = jnp.where(wave == 0.0, math.sqrt(1.0 / total), math.sqrt(2.0 / total))
    return scale * (poly * t)


def iota(shape, dim):
    return lax.broadcasted_iota(jnp.int32, shape, dim)


def split(x):
    hi = x.astype(BF16)
    return hi, (x - hi.astype(F32)).astype(BF16)


def group_masks(rows):
    lane = iota((rows, LANES), 1) // KY
    return [lane == g for g in range(LANES // KY)]


def plan(fields, n_in):
    slots = [range(f, min(f + n_in, fields)) for f in range(0, fields, n_in)]
    return slots, max(len(slots) - 2, 0)


def synthesize(coef, scale, weight_ref, row, col, numbers, variables, put):
    size, cols = coef.shape[0], col.shape[1]
    count = size // SUB
    groups = KX // SUB
    scaled = coef * scale
    stack = jnp.concatenate([jnp.where(m, scaled, 0.0) for m in group_masks(size)], axis=0)
    hi, lo = split(stack)
    lhs = jnp.concatenate([hi, lo, hi], axis=1)
    wave = jnp.dot(lhs, col, preferred_element_type=F32).reshape(groups, count, SUB, cols)
    for k, f in enumerate(numbers):
        whole = jnp.concatenate([wave[g, k] for g in range(groups)], axis=0)
        hi, lo = split(whole)
        rhs = jnp.concatenate([hi, lo, hi, lo], axis=0)
        recon = jnp.dot(row, rhs, preferred_element_type=F32)
        put(k, f, (weight_ref[f // variables] * recon).astype(BF16))


def analysis_kernel(
    dims, prog_hbm, forc_hbm, strength_hbm, level_hbm, pbl_hbm,
    coef_ref, scale_ref, weight_ref, row_ref, col_ref, early_ref,
    strength, level, pbl, prog, forc, part, mine, got_in, total, got_out, full,
    prog_sem, forc_sem, aux_sem, in_send, in_recv, out_send, out_recv, all_send, all_recv,
):
    gx, gy, n_mid, chunk = dims
    fields, rows, cols = prog.shape
    levels, variables = strength.shape
    n_chunks = fields // chunk
    groups = KX // SUB
    n_in, n_out = n_mid * gy, gx // n_mid
    slots, n_early = plan(fields, n_in)
    ix, iy = lax.axis_index("gx"), lax.axis_index("gy")
    outer, mid = ix // n_mid, lax.rem(ix, n_mid)
    me = mid * gy + iy

    def fetch(c):
        span = pl.ds(c * chunk, chunk)
        return (
            pltpu.make_async_copy(prog_hbm.at[span], prog.at[span], prog_sem.at[c]),
            pltpu.make_async_copy(forc_hbm.at[span], forc.at[span], forc_sem.at[c]),
        )

    for c in range(n_chunks):
        for copy in fetch(c):
            copy.start()
    aux = [
        pltpu.make_async_copy(pbl_hbm, pbl, aux_sem.at[0]),
        pltpu.make_async_copy(strength_hbm, strength, aux_sem.at[1]),
        pltpu.make_async_copy(level_hbm, level, aux_sem.at[2]),
    ]
    for copy in aux:
        copy.start()

    def inner_peer(d):
        other = lax.rem(me + d, n_in)
        return other, (outer * n_mid + other // gy, lax.rem(other, gy))

    def outer_peer(d):
        return (lax.rem(outer + d, n_out) * n_mid + mid, iy)

    def where_owned(s, owner, act):
        if len(slots[s]) == n_in:
            act()
        else:
            pl.when(owner < len(slots[s]))(act)

    barrier = pltpu.get_barrier_semaphore()
    for d in range(1, n_in):
        pl.semaphore_signal(barrier, inc=1, device_id=inner_peer(d)[1], device_id_type=MESH)
    for d in range(1, n_out):
        pl.semaphore_signal(barrier, inc=1, device_id=outer_peer(d), device_id_type=MESH)

    row = basis(
        rows * gx,
        (ix * rows + iota((KX, rows), 1)).astype(F32),
        iota((KX, rows), 0).astype(F32),
    )
    row_hi, row_lo = split(row)
    row_lhs = jnp.concatenate([row_hi, row_lo], axis=0)
    row_lhs = jnp.concatenate([row_lhs, row_lhs], axis=1)
    col = basis(
        cols * gy,
        (iy * cols + iota((cols, LANES), 0)).astype(F32),
        lax.rem(iota((cols, LANES), 1), KY).astype(F32),
    )
    col_rhs = jnp.concatenate(split(col), axis=1)

    def one_chunk(c, carry):
        for copy in fetch(c):
            copy.wait()
        for k in range(chunk):
            f = c * chunk + k
            diff = forc[f].astype(F32) - prog[f]
            rhs = jnp.concatenate(split(diff), axis=0)
            both = jnp.dot(row_lhs, rhs, preferred_element_type=F32)
            both = both[:KX] + both[KX:]
            for g in range(groups):
                part[g, f] = both[g * SUB:(g + 1) * SUB]
        return carry

    def to_owner(s, d):
        other, device = inner_peer(d)
        return other, pltpu.make_async_remote_copy(
            src_ref=mine.at[s, other], dst_ref=got_in.at[s, d - 1],
            send_sem=in_send.at[s, d - 1], recv_sem=in_recv.at[s, d - 1],
            device_id=device, device_id_type=MESH,
        )

    def to_plane(s, d):
        return pltpu.make_async_remote_copy(
            src_ref=total.at[s], dst_ref=got_out.at[s, d - 1],
            send_sem=out_send.at[s, d - 1], recv_sem=out_recv.at[s, d - 1],
            device_id=outer_peer(d), device_id_type=MESH,
        )

    def to_all(s, d):
        return pltpu.make_async_remote_copy(
            src_ref=full.at[s, me], dst_ref=full.at[s, me],
            send_sem=all_send.at[s, d - 1], recv_sem=all_recv.at[s, d - 1],
            device_id=inner_peer(d)[1], device_id_type=MESH,
        )

    for s, numbers in enumerate(slots):
        first, count = numbers[0], len(numbers)
        lax.fori_loop(first // chunk, (first + count) // chunk, one_chunk, 0)
        size = count * SUB
        hi, lo = split(part[:, first:first + count].reshape(groups * size, cols))
        both = jnp.dot(hi, col_rhs, preferred_element_type=F32) + jnp.dot(
            lo, col_rhs, preferred_element_type=F32
        )
        both = both[:, :LANES] + both[:, LANES:]
        coef = both[:size]
        for g, mask in list(enumerate(group_masks(size)))[1:]:
            coef = jnp.where(mask, both[g * size:(g + 1) * size], coef)
        for k in range(count):
            mine[s, k] = coef[k * SUB:(k + 1) * SUB]
        if s == 0:
            pl.semaphore_wait(barrier, n_in - 1 + n_out - 1)
        for d in range(1, n_in):
            other, copy = to_owner(s, d)
            where_owned(s, other, copy.start)

    for copy in aux:
        copy.wait()
    for l in range(levels):
        weight_ref[l] = 1.0 / (1.0 + jnp.exp(-(level[l] - pbl[...]) / RAMP_DEPTH))
        for v in range(variables):
            f = l * variables + v
            scale_ref[f * SUB:(f + 1) * SUB] = jnp.full((SUB, LANES), strength[l, v], F32)
    col_hi, col_lo = split(basis(
        cols * gy,
        (iy * cols + iota((LANES, cols), 1)).astype(F32),
        lax.rem(iota((LANES, cols), 0), KY).astype(F32),
    ))
    col_ref[...] = jnp.concatenate([col_hi, col_hi, col_lo], axis=0)
    row_hi, row_lo = split(basis(
        rows * gx,
        (ix * rows + iota((rows, 4 * KX), 0)).astype(F32),
        lax.rem(iota((rows, 4 * KX), 1), KX).astype(F32),
    ))
    row_ref[...] = jnp.where(
        iota((rows, 4 * KX), 1) < 2 * KX, row_hi.astype(F32), row_lo.astype(F32)
    ).astype(BF16)

    for s in range(len(slots)):
        def reduce_in(s=s):
            acc = mine[s, me]
            for d in range(1, n_in):
                to_owner(s, d)[1].wait_recv()
                acc = acc + got_in[s, d - 1]
            total[s] = acc
            for d in range(1, n_out):
                to_plane(s, d).start()
        where_owned(s, me, reduce_in)
    for s in range(len(slots)):
        def reduce_out(s=s):
            acc = total[s]
            for d in range(1, n_out):
                to_plane(s, d).wait_recv()
                acc = acc + got_out[s, d - 1]
            full[s, me] = acc
            for d in range(1, n_in):
                to_all(s, d).start()
        where_owned(s, me, reduce_out)
    for s, numbers in enumerate(slots):
        for d in range(1, n_in):
            sender = lax.rem(me + n_in - d, n_in)
            where_owned(s, sender, to_all(s, d).wait_recv)
        for k, f in enumerate(numbers):
            coef_ref[f * SUB:(f + 1) * SUB] = full[s, k]
        if s < n_early:
            span = slice(numbers[0] * SUB, (numbers[-1] + 1) * SUB)

            def keep(k, f, value):
                early_ref[f] = value

            synthesize(
                coef_ref[span], scale_ref[span], weight_ref, row_ref[...], col_ref[...],
                numbers, variables, keep,
            )
    for s in range(len(slots)):
        for d in range(1, n_in):
            other, copy = to_owner(s, d)
            where_owned(s, other, copy.wait_send)

        def sent(s=s):
            for d in range(1, n_out):
                to_plane(s, d).wait_send()
            for d in range(1, n_in):
                to_all(s, d).wait_send()
        where_owned(s, me, sent)


def synthesis_kernel(
    done, coef_ref, scale_ref, weight_ref, row_ref, col_ref, early_ref, tend_hbm, energy_ref,
    tend, tend_sem,
):
    levels, variables = energy_ref.shape
    fields = levels * variables

    def out(f):
        source = early_ref.at[f] if f < done else tend.at[f - done]
        return pltpu.make_async_copy(
            source, tend_hbm.at[f // variables, f % variables], tend_sem.at[f]
        )

    for f in range(done):
        out(f).start()

    def keep(k, f, value):
        tend[f - done] = value
        if k:
            out(f - 1).start()

    coef = coef_ref[...]
    synthesize(
        coef[done * SUB:], scale_ref[done * SUB:], weight_ref, row_ref[...], col_ref[...],
        range(done, fields), variables, keep,
    )
    out(fields - 1).start()

    power = coef * coef
    at_row = iota((levels, variables), 0)
    at_col = iota((levels, variables), 1)
    energy = jnp.zeros((levels, variables), F32)
    for l in range(levels):
        for v in range(variables):
            f = l * variables + v
            one = jnp.sum(power[f * SUB:(f + 1) * SUB], axis=(0, 1), keepdims=True)
            energy = jnp.where((at_row == l) & (at_col == v), one, energy)
    energy_ref[...] = energy * (1.0 / (KX * KY))

    for f in range(fields):
        out(f).wait()


def per_device(gx, gy, prognostic_values, forcing_host_values, strength, level_height, pbl_height):
    levels, variables, rows, cols = prognostic_values.shape
    fields = levels * variables
    groups = KX // SUB
    n_mid = gx
    n_in, n_out = n_mid * gy, gx // n_mid
    slots, n_early = plan(fields, n_in)
    n_slots = len(slots)
    done = n_early * n_in
    chunk = math.gcd(fields, n_in)
    n_chunks = fields // chunk
    near, far = max(n_in - 1, 1), max(n_out - 1, 1)
    anywhere = pl.BlockSpec(memory_space=pl.ANY)
    vmem = pl.BlockSpec(memory_space=pltpu.VMEM)
    dma = pltpu.SemaphoreType.DMA
    held = pl.pallas_call(
        functools.partial(analysis_kernel, (gx, gy, n_mid, chunk)),
        out_shape=(
            pltpu.VMEM((fields * SUB, LANES), F32),
            pltpu.VMEM((fields * SUB, LANES), F32),
            pltpu.VMEM((levels, rows, cols), F32),
            pltpu.VMEM((rows, 4 * KX), BF16),
            pltpu.VMEM((3 * LANES, cols), BF16),
            pltpu.VMEM((max(done, 1), rows, cols), BF16),
        ),
        in_specs=[anywhere] * 5,
        out_specs=(vmem,) * 6,
        scratch_shapes=[
            pltpu.SMEM((levels, variables), F32),
            pltpu.SMEM((levels,), F32),
            pltpu.VMEM((rows, cols), F32),
            pltpu.VMEM((fields, rows, cols), F32),
            pltpu.VMEM((fields, rows, cols), BF16),
            pltpu.VMEM((groups, fields, SUB, cols), F32),
            pltpu.VMEM((n_slots, n_in, SUB, LANES), F32),
            pltpu.VMEM((n_slots, near, SUB, LANES), F32),
            pltpu.VMEM((n_slots, SUB, LANES), F32),
            pltpu.VMEM((n_slots, far, SUB, LANES), F32),
            pltpu.VMEM((n_slots, n_in, SUB, LANES), F32),
            dma((n_chunks,)),
            dma((n_chunks,)),
            dma((3,)),
            dma((n_slots, near)),
            dma((n_slots, near)),
            dma((n_slots, far)),
            dma((n_slots, far)),
            dma((n_slots, near)),
            dma((n_slots, near)),
        ],
        compiler_params=pltpu.CompilerParams(collective_id=0, has_side_effects=True),
        name="analysis",
    )(
        prognostic_values.reshape(fields, rows, cols),
        forcing_host_values.reshape(fields, rows, cols),
        strength,
        level_height,
        pbl_height,
    )
    tendency, energy = pl.pallas_call(
        functools.partial(synthesis_kernel, done),
        out_shape=(
            jax.ShapeDtypeStruct((levels, variables, rows, cols), BF16),
            jax.ShapeDtypeStruct((levels, variables), F32),
        ),
        in_specs=[vmem] * 6,
        out_specs=(anywhere, vmem),
        scratch_shapes=[
            pltpu.VMEM((fields - done, rows, cols), BF16),
            dma((fields,)),
        ],
        name="synthesis",
    )(*[pltpu.with_memory_space_constraint(x, pltpu.VMEM) for x in held])
    return tendency, energy


def solution(mesh):
    return jax.shard_map(
        functools.partial(per_device, mesh.shape["gx"], mesh.shape["gy"]),
        mesh=mesh,
        in_specs=(P(None, None, "gx", "gy"), P(None, None, "gx", "gy"), P(), P(), P("gx", "gy")),
        out_specs=(P(None, None, "gx", "gy"), P()),
        check_vma=False,
    )
```
